32 devices in a mesh: member: 2 (over x), lon: 8 (over z, y), lat: 2 (over core).
Axes of the slice: x: 2, y: 2, z: 4, core: 2. Of those that a mesh axis runs over, the one named last changes fastest.
Arguments:
- state: float32 [128, 256, 640], P(('member', 'lat'), 'lon'), parts along dimension 0, may hold values from -6 to 6
- dep_shift: int32 [2, 128, 256], P(None, ('member', 'lat'), 'lon'), parts along dimension 1, may hold values from -8 to 8, as said below
- dep_frac: float32 [2, 128, 256], P(None, ('member', 'lat'), 'lon'), parts along dimension 1, may hold values from 0 to 1
- stiff: float32 [640], replicated, may hold values from 0.05 to 0.2
Outputs:
- advanced: float32 [128, 256, 640], P(('member', 'lat'), 'lon'), parts along dimension 0
The draws below stay inside these ranges and needn't reach their ends.
There are 2 independent parts, one for each index of `member`. The reference program is written for one: setup_inputs(seed, part) draws one part's arguments, and reference() takes and returns one part's arrays. A program takes and returns all parts, laid end to end along the dimension named above; an argument that names none is the same for every part. Nothing has to cross between parts.
Inputs may be any that keep to these rules, and one draw needn't show every extreme that they name: `dep_shift`: both ends of the range are taken in every draw; the spread of displacements differs from row to row.
All inputs are finite; a program needn't handle non-finite values.
Results may differ from the reference program's by a relative error of at most 0.00007.
Values sent between devices are 32-bit elements; how exact they have to be, the bound alone decides.
A program may use at most 64 MiB of HBM per device.

```python
import math
import jax
import jax.numpy as jnp

FIELDS = 5
LEV = 128
TRAJ = 2
REACH = 8
FL = 640
NLAT = 64
NLON = 256


def draw_dep_shift(key, part):
    first = jax.random.fold_in(key, 11)
    second = jax.random.fold_in(key, 23)
    speed = jax.random.randint(first, (TRAJ, NLAT, 1), 1, REACH + 1)
    raw = jax.random.randint(second, (TRAJ, NLAT, NLON), 0 - REACH, REACH + 1)
    shift = jnp.clip(raw, -speed, speed)
    shift = shift.at[:, 0, 0].set(0 - REACH)
    shift = shift.at[:, -1, -1].set(REACH)
    return shift.astype(jnp.int32)


def block_scale(key, extent, shards, least, high):
    gain, own = 1.0, jax.random.fold_in(key, 6)
    for dim, shards_of in shards:
        draws = jnp.exp(jax.random.uniform(jax.random.fold_in(own, dim), (shards_of,), jnp.float32, least / len(shards), high / len(shards)))
        gain = gain * jnp.repeat(draws, extent[dim] // shards_of).reshape([-1 if axis == dim else 1 for axis in range(len(extent))])
    return gain


def centred(own_key, extent, spread, reach, split=(), kind=jnp.bfloat16):
    entries = spread * jax.random.normal(own_key, extent, jnp.float32)
    if split:
        entries = entries * block_scale(own_key, extent, split, -0.22, 0.18)
    return jnp.clip(entries, -reach, reach).astype(kind)


def setup_inputs(seed: int = 0, part: int = 0) -> dict:
    seeds = jax.random.split(jax.random.key(seed), 5)
    part_splits = jax.random.split(jax.random.fold_in(seeds[4], part), 5)
    state = centred(part_splits[0], (NLAT, NLON, FL), 1.0, 6.0, ((0, 2), (1, 8)), jnp.float32)
    dep_shift = draw_dep_shift(jax.random.fold_in(jax.random.fold_in(seeds[4], part), 71), part)
    dep_frac = jnp.clip(1.0 * jax.random.uniform(part_splits[2], (TRAJ, NLAT, NLON), jnp.float32) ** block_scale(part_splits[2], (TRAJ, NLAT, NLON), ((1, 2), (2, 8)), -0.2, 0.2), 0.0, 1.0)
    stiff = jnp.clip(jnp.exp(jax.random.uniform(seeds[3], (FL,), jnp.float32, math.log(0.05), math.log(0.2))), 0.05, 0.2)
    return {"state": state, "dep_shift": dep_shift, "dep_frac": dep_frac, "stiff": stiff}


OMEGAS = (0.4227, 0.8104)


def vertical(rows, frac):
    shaped = rows.reshape(rows.shape[:-1] + (FIELDS, LEV))
    upper = jnp.concatenate([shaped[..., 1:], shaped[..., -1:]], axis=-1)
    mixed = shaped + frac[..., None, None] * (upper - shaped)
    return mixed.reshape(rows.shape)


def sweep(field, rhs, stiff, omega):
    east = jnp.roll(field, -1, axis=1)
    west = jnp.roll(field, 1, axis=1)
    blank = jnp.zeros_like(field[:1])
    north = jnp.concatenate([field[1:], blank], axis=0)
    south = jnp.concatenate([blank, field[:-1]], axis=0)
    lap = ((south + north) + (west + east)) - 4.0 * field
    resid = rhs - (field - stiff * lap)
    return field + omega * resid


def reference(state, dep_shift, dep_frac, stiff):
    lon_index = jnp.arange(NLON, dtype=jnp.int32)[None, :]
    field = state
    for turn in range(TRAJ):
        src_lon = (lon_index + dep_shift[turn]) % NLON
        upstream = jnp.take_along_axis(state, src_lon[:, :, None].astype(jnp.int32), axis=1)
        rhs = vertical(upstream, dep_frac[turn])
        for which in range(2):
            field = sweep(field, rhs, stiff, OMEGAS[which])
    return field
```

```python
import functools

import jax
import jax.numpy as jnp
from jax import lax
from jax.experimental import pallas as pl
from jax.experimental.pallas import tpu as pltpu
from jax.sharding import PartitionSpec as P

LEV = 128
REACH = 8
OMEGAS = (0.4227, 0.8104)
CH = 4
MSG = 4
STEP = 2
DEEP = REACH + 3
PAD = 16
SKIRT = 4
LEAD = 12
GROW = 1
MESH = pl.DeviceIdType.MESH


def kernel(lons, state, shift_in, share_in, stiff_in, out, shift, share, stiff, ext, xa, xb, xc, ra, rb, deps,
           small_sem, load_sem, send_sem, recv_sem, dep_send, dep_recv, lat_send, lat_recv, far_sem):
    rows, cols, width = state.shape
    fields = width // LEV
    chunks = rows // MSG
    wide = cols + 2 * PAD
    win = cols + 2 * SKIRT
    edge = PAD - SKIRT
    me = lax.axis_index("lon")
    lat = lax.axis_index("lat")
    south = lat == 0
    right, left = lax.rem(me + 1, lons), lax.rem(me + lons - 1, lons)
    peer = 1 - lat

    even = lax.rem(me, 2) == 0
    near = jnp.where(even, right, left)
    far = jnp.where(even, left, right)
    early = jnp.logical_or(me == 0, jnp.logical_and(jnp.logical_not(even), me != lons - 1))
    barrier = pltpu.get_barrier_semaphore()
    for where in ({"lon": near}, {"lat": peer}):
        pl.semaphore_signal(barrier, inc=1, device_id=where, device_id_type=MESH)

    @pl.when(early)
    def _():
        pl.semaphore_signal(barrier, inc=1, device_id={"lon": far}, device_id_type=MESH)

    def phys(j):
        return jnp.where(south, rows - 1 - j, j) + CH

    def block(lo, n):
        return pl.ds(jnp.where(south, rows - lo - n, lo) + CH, n)

    def load(c):
        start = jnp.where(south, rows - MSG - MSG * c, MSG * c)
        for f in range(fields):
            pltpu.make_async_copy(
                state.at[pl.ds(start, MSG), :, f * LEV:(f + 1) * LEV],
                ext.at[pl.ds(start + CH, MSG), f, PAD:PAD + cols, :],
                load_sem.at[c]).start()

    def arrived(ref, sem):
        pltpu.make_async_copy(ref, ref, sem).wait()

    def loaded(c):
        arrived(ext.at[block(MSG * c, MSG), :, PAD:PAD + cols, :], load_sem.at[c])

    load(0)
    sends = []

    def send(src, dst, ssem, rsem, where):
        copy = pltpu.make_async_remote_copy(
            src_ref=src, dst_ref=dst, send_sem=ssem, recv_sem=rsem,
            device_id=where, device_id_type=MESH)
        copy.start()
        sends.append(copy)

    spans = message_spans(rows, fields)
    messages = len(spans)

    def lon_copy(side, c):
        lo, hi, f0, f1 = spans[c]
        here = block(lo, hi - lo)
        if side == 0:
            src, dst, where = PAD + cols - DEEP, PAD - DEEP, right
        else:
            src, dst, where = PAD, PAD + cols, left
        return pltpu.make_async_remote_copy(
            src_ref=ext.at[here, f0:f1, src:src + DEEP, :],
            dst_ref=ext.at[here, f0:f1, dst:dst + DEEP, :],
            send_sem=send_sem.at[side], recv_sem=recv_sem.at[side, c],
            device_id={"lon": where}, device_id_type=MESH)

    def ahead(r):
        return LEAD + GROW * r

    def dep_copy(side):
        src, dst, where = ((PAD + cols - 8, PAD - 8, right), (PAD, PAD + cols, left))[side]
        return pltpu.make_async_remote_copy(
            src_ref=deps.at[0, src:src + 8, :], dst_ref=deps.at[0, dst:dst + 8, :],
            send_sem=dep_send.at[side], recv_sem=dep_recv.at[side],
            device_id={"lon": where}, device_id_type=MESH)

    def first(longer):
        lon_copy(1 - longer, 0).start()

    def issue(longer):
        dep_copy(1 - longer).start()
        for c in range(messages):
            if c and spans[c][0] % MSG == 0 and spans[c][2] == 0:
                loaded(spans[c][0] // MSG)
            if c:
                lon_copy(1 - longer, c).start()

    def open_long(longer):
        dep_copy(longer).start()
        for c in range(messages):
            if spans[c][0] < ahead(0):
                lon_copy(longer, c).start()

    def follow(c):
        lo, hi, f0, _ = spans[c]
        then = [m for m, span in enumerate(spans) if ahead(lo) <= span[0] < ahead(hi)]

        def step(longer):
            for m in then:
                lon_copy(longer, m).start()

        if f0 == 0 and then:
            pl.when(even)(functools.partial(step, 1))
            pl.when(jnp.logical_not(even))(functools.partial(step, 0))

    smalls = []
    for i, (src, dst) in enumerate(((shift_in, shift), (share_in, share), (stiff_in, stiff))):
        smalls.append(pltpu.make_async_copy(src, dst, small_sem.at[i]))
        smalls[-1].start()
    with jax.named_scope("bar"):
        pl.semaphore_wait(barrier, jnp.where(early, 2, 3))

        @pl.when(jnp.logical_not(early))
        def _():
            pl.semaphore_signal(far_sem, inc=1, device_id={"lon": far}, device_id_type=MESH)
    with jax.named_scope("load0"):
        loaded(0)
    pl.when(even)(functools.partial(first, 1))
    pl.when(jnp.logical_not(even))(functools.partial(first, 0))
    for c in range(1, chunks):
        load(c)
    for copy in smalls:
        copy.wait()
    dep = jnp.concatenate(
        [shift[...].astype(jnp.float32).reshape(2 * rows, cols), share[...].reshape(2 * rows, cols)],
        axis=0).T
    deps[0, PAD:PAD + cols, :] = dep
    with jax.named_scope("issue"):
        pl.when(even)(functools.partial(issue, 1))
        pl.when(jnp.logical_not(even))(functools.partial(issue, 0))
    with jax.named_scope("far"):
        pl.when(early)(lambda: pl.semaphore_wait(far_sem, 1))
    pl.when(even)(functools.partial(open_long, 1))
    pl.when(jnp.logical_not(even))(functools.partial(open_long, 0))

    zero = jnp.zeros((fields, PAD - DEEP, LEV), jnp.float32)

    def blank_cols(i, _):
        ext[i, :, 0:PAD - DEEP, :] = zero
        ext[i, :, wide - PAD + DEEP:wide, :] = zero
        return 0

    lax.fori_loop(0, rows + 2 * CH, blank_cols, 0)
    beyond = phys(rows)
    for buf in (ext, xa, xb, xc):
        buf[beyond] = jnp.zeros((fields, wide, LEV), jnp.float32)

    sides = ((PAD - DEEP, PAD), (PAD + cols, PAD + cols + DEEP))
    dep_sides = ((PAD - 8, PAD), (PAD + cols, PAD + cols + 8))

    def wait_chunk(c):
        lo, hi, f0, f1 = spans[c]
        with jax.named_scope(f"w{hi}"):
            here = block(lo, hi - lo)
            for side, (first, last) in enumerate(sides):
                arrived(ext.at[here, f0:f1, first:last, :], recv_sem.at[side, c])
        follow(c)

    there = pl.ds(jnp.where(south, 0, rows + CH), CH)
    here = pl.ds(jnp.where(south, rows + CH, 0), CH)
    with jax.named_scope("dep"):
        for side, (lo, hi) in enumerate(dep_sides):
            arrived(deps.at[0, lo:hi, :], dep_recv.at[side])
    span = slice(PAD - 8, PAD + cols + 8)
    full = slice(PAD - DEEP, PAD + cols + DEEP)
    send(deps.at[0, span, :], deps.at[1, span, :], lat_send.at[0], lat_recv.at[0], {"lat": peer})
    heads = [c for c, span in enumerate(spans) if span[0] < CH]
    for c in heads:
        wait_chunk(c)
    send(ext.at[block(0, CH), :, full, :], ext.at[there, :, full, :], lat_send.at[1], lat_recv.at[1], {"lat": peer})
    with jax.named_scope("lat"):
        arrived(deps.at[1, span, :], lat_recv.at[0])
        arrived(ext.at[here, :, full, :], lat_recv.at[1])

    lane_k = lax.broadcasted_iota(jnp.int32, (win, 2 * wide), 1)
    lane_k = jnp.where(lane_k >= wide, lane_k - wide, lane_k).astype(jnp.float32)
    col_q = (lax.broadcasted_iota(jnp.int32, (win, 1), 0) + edge).astype(jnp.float32)
    top = lax.broadcasted_iota(jnp.int32, (win, LEV), 1) == LEV - 1

    def interpolate(j, f0, f1):
        ups = []
        for r in range(STEP):
            p = phys(j + r)
            lane = lax.rem(p - CH + rows, rows)
            table = deps[jnp.where(j < 0, 1, 0), edge:edge + win, :]
            table = pltpu.roll(table, lax.rem(4 * rows - lane, 4 * rows), 1)
            picks = [
                jnp.where(lane_k == table[:, t * rows:t * rows + 1] + col_q, 1.0, 0.0)
                for t in range(2)
            ]
            picker = jnp.concatenate(picks, axis=0).astype(jnp.bfloat16)
            parts = []
            for f in range(f0, f1):
                val = ext[p, f]
                high = val.astype(jnp.bfloat16)
                low = (val - high.astype(jnp.float32)).astype(jnp.bfloat16)
                parts.append(jnp.concatenate([high, low], axis=0))
            up = jnp.dot(picker, jnp.concatenate(parts, axis=1),
                         preferred_element_type=jnp.float32)
            ups.append((p, table, up))
        for p, table, up in ups:
            for t, rhs in enumerate((ra, rb)):
                frac = table[:, (2 + t) * rows:(2 + t) * rows + 1]
                for f in range(f0, f1):
                    u = up[t * win:(t + 1) * win, (f - f0) * LEV:(f - f0 + 1) * LEV]
                    above = jnp.where(top, u, pltpu.roll(u, LEV - 1, 1))
                    rhs[p, f] = u + frac * (above - u)

    def sweep(j, n_rows, f0, f1, src, rhs, dst, omega, last=False):
        lo, n = (PAD, cols) if last else (edge, win)
        for f in range(f0, f1):
            coef = omega * stiff[pl.ds(f * LEV, LEV)].reshape(1, LEV)
            for r in range(n_rows):
                p, north, below = phys(j + r), phys(j + r + 1), phys(j + r - 1)
                around = (src[north, f, lo:lo + n, :] + src[below, f, lo:lo + n, :]) + (
                    src[p, f, lo - 1:lo - 1 + n, :] + src[p, f, lo + 1:lo + 1 + n, :])
                new = ((1.0 - omega) - 4.0 * coef) * src[p, f, lo:lo + n, :] + (
                    coef * around + omega * rhs[p, f, lo - edge:lo - edge + n, :])
                if last:
                    out[p - CH, :, f * LEV:(f + 1) * LEV] = new
                else:
                    dst[p, f, lo:lo + n, :] = new

    sweeps = (
        lambda j, n, f0, f1: sweep(j, n, f0, f1, ext, ra, xa, OMEGAS[0]),
        lambda j, n, f0, f1: sweep(j, n, f0, f1, xa, ra, xb, OMEGAS[1]),
        lambda j, n, f0, f1: sweep(j, n, f0, f1, xb, rb, xc, OMEGAS[0]),
        lambda j, n, f0, f1: sweep(j, n, f0, f1, xc, rb, None, OMEGAS[1], True),
    )

    def advance(j, deep, f0, f1):
        interpolate(j, f0, f1)
        for k in range(deep):
            sweeps[k](j - 1 - k, STEP, f0, f1)

    with jax.named_scope("opening"):
        for k in range(4):
            advance(STEP * k - CH, k, 0, fields)

    for c, (lo, hi, f0, f1) in enumerate(spans):
        if c in heads:
            continue
        wait_chunk(c)
        if hi - lo == STEP:
            advance(lo, 4, f0, f1)
        else:
            def pair(i, _):
                advance(STEP * i, 4, 0, fields)
                return 0

            lax.fori_loop(lo // STEP, hi // STEP, pair, 0)
        if hi == rows:
            with jax.named_scope("tail"):
                for k in range(4):
                    done = rows - 1 - k
                    while done < rows:
                        n = min(STEP, rows - done)
                        sweeps[k](done, n, f0, f1)
                        done += n
    with jax.named_scope("drain"):
        for copy in sends:
            copy.wait_send()
        for side in range(2):
            dep_copy(side).wait_send()
        for side, (first_col, last_col) in enumerate(sides):
            arrived(ext.at[CH:CH + rows, :, first_col:last_col, :], send_sem.at[side])


def message_spans(rows, fields):
    spans, lo = [], 0
    while lo < rows - STEP:
        size = MSG if lo < rows - BY_STEP else STEP
        spans.append((lo, lo + size, 0, fields))
        lo += size
    cuts = (0, fields - LATE, fields)
    return spans + [(lo, rows, first, last) for first, last in zip(cuts, cuts[1:])]


BY_STEP = 16
LATE = 2


def shards(lons, state, dep_shift, dep_frac, stiff):
    rows, cols, width = state.shape
    fields = width // LEV
    state, dep_shift, dep_frac, stiff = (
        pltpu.with_memory_space_constraint(x, pltpu.HBM) for x in (state, dep_shift, dep_frac, stiff))
    wide = cols + 2 * PAD
    padded = pltpu.VMEM((rows + 2 * CH, fields, wide, LEV), jnp.float32)
    rhs = pltpu.VMEM((rows + 2 * CH, fields, cols + 2 * SKIRT, LEV), jnp.float32)
    dma = pltpu.SemaphoreType.DMA
    messages = len(message_spans(rows, fields))
    vmem = pl.BlockSpec(memory_space=pltpu.VMEM)
    return pl.pallas_call(
        functools.partial(kernel, lons),
        out_shape=jax.ShapeDtypeStruct(state.shape, jnp.float32),
        in_specs=[pl.BlockSpec(memory_space=pltpu.HBM)] * 4,
        out_specs=vmem,
        scratch_shapes=[
            pltpu.VMEM(dep_shift.shape, jnp.int32), pltpu.VMEM(dep_frac.shape, jnp.float32),
            pltpu.VMEM(stiff.shape, jnp.float32),
            padded, padded, padded, padded, rhs, rhs,
            pltpu.VMEM((2, wide, 4 * rows), jnp.float32),
            dma((3,)), dma((rows // MSG,)), dma((2,)), dma((2, messages)),
            dma((2,)), dma((2,)), dma((2,)), dma((2,)), pltpu.SemaphoreType.REGULAR,
        ],
        compiler_params=pltpu.CompilerParams(collective_id=0, has_side_effects=True, vmem_limit_bytes=42 << 20),
    )(state, dep_shift, dep_frac, stiff)


def solution(mesh):
    in_specs = (
        P(("member", "lat"), "lon", None),
        P(None, ("member", "lat"), "lon"),
        P(None, ("member", "lat"), "lon"),
        P(),
    )
    out_specs = P(("member", "lat"), "lon", None)
    if mesh.shape["lat"] != 2 or mesh.shape["lon"] % 2 or mesh.shape["lon"] < 4:
        raise ValueError("unsupported mesh")
    body = functools.partial(shards, mesh.shape["lon"])
    return jax.shard_map(body, mesh=mesh, in_specs=in_specs, out_specs=out_specs, check_vma=False)
```
